32 devices in a mesh: seq: 8 (over z, y), head: 4 (over x, core).
Axes of the slice: x: 2, y: 2, z: 4, core: 2. Of those that a mesh axis runs over, the one named last changes fastest.
Arguments:
- tokens: bfloat16 [6144, 2560], P(('seq', 'head')), may hold values from -12 to 12
- pre_gain: float32 [2560], replicated, may hold values from 0.25 to 1.75
- inner_proj: bfloat16 [2560, 2, 5120], P(None, None, 'head'), may hold values from -0.125 to 0.125
- outer_proj: bfloat16 [2560, 336], replicated, may hold values from -0.125 to 0.125
- kernel_x: float32 [4, 5120], P(None, 'head'), may hold values from -3 to 3
- kernel_bc: float32 [4, 256], replicated, may hold values from -3 to 3
- offset_x: float32 [5120], P('head'), may hold values from -3 to 3
- offset_bc: float32 [256], replicated, may hold values from -3 to 3
- dt_bias: float32 [80], P('head'), may hold values from -7 to -5
- a_log: float32 [80], P('head'), may hold values from -12 to 4
- skip_gain: float32 [80], P('head'), may hold values from 0.5 to 1.5
- norm_gain: float32 [5120], P('head'), may hold values from 0.25 to 1.75
- out_proj: bfloat16 [5120, 2560], P('head'), may hold values from -0.078125 to 0.078125
Outputs:
- mixed: bfloat16 [6144, 2560], P(('seq', 'head'))
The draws below stay inside these ranges and needn't reach their ends.
All inputs are finite; a program needn't handle non-finite values.
Results may differ from the reference program's by a relative error of at most 0.014.
Values may be sent and summed in bfloat16 or wider, within the bound.
A program may use at most 128 MiB of HBM per device.

```python
import jax
import jax.numpy as jnp
from jax import lax

D = 2560
H = 80
P_SIZE = 64
N = 128
CONV = 4
SPAN = 256
DI = 5120
TOKENS = 6144
N_HEAD = 4


def draw_tokens(key, part):
    noise_key, level_key, course_key = jax.random.split(key, 3)
    blocks = TOKENS // SPAN
    noise = jax.random.normal(noise_key, (TOKENS, D), jnp.float32)
    levels = 2.0 * jax.random.normal(level_key, (blocks, 1, 1), jnp.float32)
    course = jax.random.normal(course_key, (1, 1, D), jnp.float32)
    shifted = noise.reshape(blocks, SPAN, D) + levels * course
    return jnp.clip(shifted.reshape(TOKENS, D), -12.0, 12.0).astype(jnp.bfloat16)


def draw_a_log(key, part):
    order_key, rate_key = jax.random.split(key)
    order = jax.random.permutation(order_key, H)
    share = H // 2
    quick = order < share
    spread = jax.random.uniform(rate_key, (H,), jnp.float32)
    quick_rate = jnp.log(4.0) + spread * jnp.log(10.0)
    patient_rate = jnp.log(10.0 / TOKENS) + spread * jnp.log(10.0)
    return jnp.where(quick, quick_rate, patient_rate).astype(jnp.float32)


def block_levels(own_key, dims, cuts, least, top_value):
    level = 1.0
    for dim, blocks in cuts:
        heights = jax.random.uniform(jax.random.fold_in(jax.random.fold_in(own_key, 6), dim), (blocks,), jnp.float32, least / len(cuts), top_value / len(cuts))
        level = level * jnp.repeat(jnp.exp(heights), dims[dim] // blocks).reshape((-1,) + (1,) * (len(dims) - 1 - dim))
    return level


def normal_values(stream_key, dims, scale, limit, cuts=(), kind=jnp.bfloat16):
    drawn = jax.random.normal(stream_key, dims, jnp.float32) * scale
    if len(cuts) > 0:
        drawn = block_levels(stream_key, dims, cuts, -0.22, 0.18) * drawn
    return jnp.clip(drawn, min=-limit, max=limit).astype(kind)


def setup_inputs(seed: int = 0) -> dict:
    streams_of = jax.random.split(jax.random.key(seed), 14)
    tokens = draw_tokens(jax.random.fold_in(streams_of[13], 71), 0)
    pre_gain = jnp.clip(1.0 + 0.15 * jax.random.normal(streams_of[1], (D,), jnp.float32), 0.25, 1.75)
    inner_proj = normal_values(streams_of[2], (D, 2, DI), D ** -0.5, 0.125, ((2, 4),))
    outer_proj = normal_values(streams_of[3], (D, 2 * N + H), D ** -0.5, 0.125)
    kernel_x = normal_values(streams_of[4], (CONV, DI), CONV ** -0.5, 3.0, ((1, 4),), jnp.float32)
    kernel_bc = normal_values(streams_of[5], (CONV, 2 * N), CONV ** -0.5, 3.0, (), jnp.float32)
    offset_x = normal_values(streams_of[6], (DI,), 0.5, 3.0, ((0, 4),), jnp.float32)
    offset_bc = normal_values(streams_of[7], (2 * N,), 0.5, 3.0, (), jnp.float32)
    dt_bias = jnp.clip(-7.0 + 2.0 * jax.random.uniform(streams_of[8], (H,), jnp.float32) ** block_levels(streams_of[8], (H,), ((0, 4),), -0.2, 0.2), -7.0, -5.0)
    a_log = draw_a_log(jax.random.fold_in(streams_of[13], 71), 0)
    skip_gain = jnp.clip(0.5 + 1.0 * jax.random.uniform(streams_of[10], (H,), jnp.float32) ** block_levels(streams_of[10], (H,), ((0, 4),), -0.2, 0.2), 0.5, 1.5)
    norm_gain = jnp.clip(1.0 + 0.15 * jax.random.normal(streams_of[11], (DI,), jnp.float32), 0.25, 1.75)
    out_proj = normal_values(streams_of[12], (DI, D), DI ** -0.5, 0.078125, ((0, 4),))
    return {"tokens": tokens, "pre_gain": pre_gain, "inner_proj": inner_proj, "outer_proj": outer_proj, "kernel_x": kernel_x, "kernel_bc": kernel_bc, "offset_x": offset_x, "offset_bc": offset_bc, "dt_bias": dt_bias, "a_log": a_log, "skip_gain": skip_gain, "norm_gain": norm_gain, "out_proj": out_proj}


norm_floor = 0.1

def row_norm(row_block, gain_vector):
    widened = row_block.astype(jnp.float32)
    inverse_rms = lax.rsqrt(lax.optimization_barrier(jnp.mean(widened * widened, axis=-1, keepdims=True)) + norm_floor)
    return widened * inverse_rms * gain_vector

def masked_exp(log_gap, causal):
    return jnp.where(causal, jnp.exp(jnp.where(causal, log_gap, 0.0)), 0.0)

def block_scan(values_x, values_b, values_c, step_sizes, decay_rate, ssm_state):
    running = jnp.cumsum(step_sizes * decay_rate, axis=0)
    score_rows = jnp.dot(values_c, values_b.T, preferred_element_type=jnp.float32)
    running_heads = running.T
    row_index = lax.broadcasted_iota(jnp.int32, (SPAN, SPAN), 0)
    col_index = lax.broadcasted_iota(jnp.int32, (SPAN, SPAN), 1)
    decay_factor = masked_exp(running_heads[:, :, None] - running_heads[:, None, :], row_index >= col_index)
    mix_weights = (score_rows[None] * decay_factor * step_sizes.T[:, None, :]).astype(jnp.bfloat16)
    intra_out = jnp.einsum('hts,shp->thp', mix_weights.astype(jnp.float32), values_x.astype(jnp.float32))
    end_weight = jnp.exp(running[-1:] - running) * step_sizes
    scaled_x = (values_x.astype(jnp.float32) * end_weight[:, :, None]).astype(jnp.bfloat16)
    block_state = jnp.einsum('shp,sn->hpn', scaled_x.astype(jnp.float32), values_b.astype(jnp.float32))
    cross_out = jnp.exp(running)[:, :, None] * jnp.einsum('tn,hpn->thp', values_c.astype(jnp.float32), ssm_state, precision=lax.Precision.HIGHEST)
    next_state = jnp.exp(running[-1])[:, None, None] * ssm_state + block_state
    return (intra_out + cross_out, next_state)

def reference(tokens, pre_gain, inner_proj, outer_proj, kernel_x, kernel_bc, offset_x, offset_bc, dt_bias, a_log, skip_gain, norm_gain, out_proj):
    decay_rate = -jnp.exp(a_log)
    joined_proj = inner_proj.reshape(D, 2 * DI)
    conv_weight = jnp.concatenate([kernel_x, kernel_bc], axis=1)
    conv_bias = jnp.concatenate([offset_x, offset_bc])
    group_width = DI // N_HEAD

    def advance(carry, row_block):
        ssm_state, conv_tail = carry
        normed = row_norm(row_block, pre_gain).astype(jnp.bfloat16)
        inner_part = jnp.dot(normed, joined_proj, preferred_element_type=jnp.float32)
        outer_part = jnp.dot(normed, outer_proj, preferred_element_type=jnp.float32)
        gate_in = inner_part[:, :DI].astype(jnp.bfloat16)
        x_in = inner_part[:, DI:].astype(jnp.bfloat16)
        bc_in = outer_part[:, :2 * N].astype(jnp.bfloat16)
        dt_raw = outer_part[:, 2 * N:]
        conv_input = jnp.concatenate([x_in, bc_in], axis=1)
        extended = jnp.concatenate([conv_tail, conv_input], axis=0)
        summed = jnp.broadcast_to(conv_bias, conv_input.shape).astype(jnp.float32)
        for offset in range(CONV):
            summed = summed + conv_weight[offset] * extended[offset:offset + SPAN].astype(jnp.float32)
        conv_out = jax.nn.silu(summed).astype(jnp.bfloat16)
        values_x = conv_out[:, :DI].reshape(SPAN, H, P_SIZE)
        values_b = conv_out[:, DI:DI + N]
        values_c = conv_out[:, DI + N:]
        step_sizes = jax.nn.softplus(dt_raw + dt_bias)
        scan_out, next_state = block_scan(values_x, values_b, values_c, step_sizes, decay_rate, ssm_state)
        mixer_out = (scan_out + skip_gain[:, None] * values_x.astype(jnp.float32)).reshape(SPAN, DI)
        gated = mixer_out * jax.nn.silu(gate_in.astype(jnp.float32))
        normed_out = row_norm(gated, norm_gain).astype(jnp.bfloat16)
        total = jnp.zeros((SPAN, D), jnp.float32)
        for offset in range(N_HEAD):
            lower = offset * group_width
            partial_value = jnp.dot(normed_out[:, lower:lower + group_width], out_proj[lower:lower + group_width], preferred_element_type=jnp.float32).astype(jnp.bfloat16)
            total = total + lax.optimization_barrier(partial_value).astype(jnp.float32)
        next_tail = extended[SPAN:]
        return ((next_state, next_tail), total.astype(jnp.bfloat16))
    start_state = jnp.zeros((H, P_SIZE, N), jnp.float32)
    start_tail = jnp.zeros((CONV - 1, DI + 2 * N), jnp.bfloat16)
    blocks_in = tokens.reshape(TOKENS // SPAN, SPAN, D)
    final_carry, outputs = lax.scan(advance, (start_state, start_tail), blocks_in)
    return outputs.reshape(TOKENS, D)
```

```python
import functools

import jax
import jax.numpy as jnp
from jax import lax
from jax.experimental import pallas as pl
from jax.experimental.pallas import tpu as pltpu
from jax.sharding import PartitionSpec as P

SPAN = 256
HALO = 16
LANES = 128


norm_floor = 0.1


def row_norm(row_block, gain_vector):
    widened = row_block.astype(jnp.float32)
    inverse_rms = lax.rsqrt(jnp.mean(widened * widened, axis=-1, keepdims=True) + norm_floor)
    return widened * inverse_rms * gain_vector


def silu(value):
    return value * (1.0 / (1.0 + jnp.exp(-value)))


def exact_dot(a, b):
    return jnp.dot(a, b, precision=lax.Precision.HIGHEST, preferred_element_type=jnp.float32)


def scan_kernel(
    sizes,
    inner_ref,
    bc_ref,
    dt_ref,
    kernel_x_ref,
    offset_x_ref,
    kernel_bc_ref,
    offset_bc_ref,
    rate_ref,
    skip_ref,
    gain_ref,
    out_ref,
    halo_x,
    halo_bc,
    ext_x,
    ext_bc,
    conv_x,
    conv_bc,
    y_buf,
    cum_buf,
    states,
    carried,
    sum_out,
    sum_in,
    rate_out,
    rate_in,
    carry_out,
    carry_in,
    sq_out,
    sq_in,
    halo_sems,
    sum_send,
    sum_recv,
    rate_send,
    rate_recv,
    carry_send,
    carry_recv,
    sq_send,
    sq_recv,
):
    devices, groups, rows, width, state, taps, head_size = sizes
    blocks = rows // SPAN
    share = state // devices
    total_width = width * groups
    me = lax.axis_index("seq")
    group = lax.axis_index("head")
    seq_peer = [lax.rem(me + o, devices) for o in range(devices)]
    seq_back = [lax.rem(me - o + devices, devices) for o in range(devices)]
    head_peer = [lax.rem(group + o, groups) for o in range(groups)]

    barrier = pltpu.get_barrier_semaphore()
    for o in range(1, devices):
        pl.semaphore_signal(barrier, 1, device_id={"seq": seq_peer[o]})
    for o in range(1, groups):
        pl.semaphore_signal(barrier, 1, device_id={"head": head_peer[o]})
    pl.semaphore_wait(barrier, devices + groups - 2)

    def remote(src, dst, send, recv, axis, peer):
        copy = pltpu.make_async_remote_copy(
            src_ref=src, dst_ref=dst, send_sem=send, recv_sem=recv, device_id={axis: peer}
        )
        return copy

    halo_copies = [
        remote(
            inner_ref.at[pl.ds(rows - HALO, HALO), pl.ds(width, width)],
            halo_x, halo_sems.at[0], halo_sems.at[1], "seq", seq_peer[1],
        ),
        remote(
            bc_ref.at[pl.ds(rows - HALO, HALO), :],
            halo_bc, halo_sems.at[2], halo_sems.at[3], "seq", seq_peer[1],
        ),
    ]
    for copy in halo_copies:
        copy.start()

    def widen(k, carry):
        row = pl.multiple_of(k * 64, 64)
        ext_x[pl.ds(8 + row, 64), :] = inner_ref[pl.ds(row, 64), pl.ds(width, width)].astype(
            jnp.float32
        )
        ext_bc[pl.ds(8 + row, 64), :] = bc_ref[pl.ds(row, 64), :].astype(jnp.float32)
        return carry

    lax.fori_loop(0, rows // 64, widen, 0)
    for copy in halo_copies:
        copy.wait()
    first = me > 0
    ext_x[0:8, :] = jnp.where(first, halo_x[...].astype(jnp.float32)[HALO - 8 :], 0.0)
    ext_bc[0:8, :] = jnp.where(first, halo_bc[...].astype(jnp.float32)[HALO - 8 :], 0.0)

    def convolve(source, weight, bias, target, columns):
        def step(k, carry):
            row = pl.multiple_of(k * 32, 32)
            for lower in range(0, columns, LANES):
                lanes = pl.ds(lower, LANES)
                window = source[pl.ds(row, 40), lanes]
                total = jnp.broadcast_to(bias[0:1, lanes], (32, LANES))
                for tap in range(taps):
                    shift = 8 - taps + 1 + tap
                    total = total + weight[tap : tap + 1, lanes] * window[shift : shift + 32]
                target[pl.ds(row, 32), lanes] = silu(total).astype(jnp.bfloat16)
            return carry

        lax.fori_loop(0, rows // 32, step, 0)

    convolve(ext_bc, kernel_bc_ref, offset_bc_ref, conv_bc, 2 * state)
    convolve(ext_x, kernel_x_ref, offset_x_ref, conv_x, width)

    head_of_lane = lax.broadcasted_iota(jnp.int32, (LANES, width), 1) // head_size
    spread = (head_of_lane == lax.broadcasted_iota(jnp.int32, (LANES, width), 0)).astype(
        jnp.float32
    )
    lower_tri = (
        lax.broadcasted_iota(jnp.int32, (SPAN, SPAN), 0)
        >= lax.broadcasted_iota(jnp.int32, (SPAN, SPAN), 1)
    ).astype(jnp.float32)

    states[0] = jnp.zeros((state, width), jnp.float32)
    prefix = jnp.zeros((1, LANES), jnp.float32)
    prefixes = []
    for block in range(blocks):
        span = pl.ds(block * SPAN, SPAN)
        step_sizes = dt_ref[span, :]
        running = exact_dot(lower_tri, step_sizes * rate_ref[...])
        cum_buf[span, :] = running
        last = running[SPAN - 1 : SPAN, :]
        end_weight = exact_dot(jnp.exp(last - running) * step_sizes, spread)
        scaled = (conv_x[span, :].astype(jnp.float32) * end_weight).astype(jnp.bfloat16)
        new_state = lax.dot_general(
            conv_bc[span, pl.ds(0, state)], scaled, (((0,), (0,)), ((), ())),
            preferred_element_type=jnp.float32,
        )
        decay = exact_dot(jnp.broadcast_to(jnp.exp(last), (8, LANES)), spread)[0:1]
        states[block + 1] = decay * states[block] + new_state
        prefixes.append(prefix)
        prefix = prefix + last

    for j in range(devices):
        sum_out[j] = states[blocks, pl.ds(j * share, share), :].astype(jnp.bfloat16)
    rate_out[...] = jnp.broadcast_to(prefix, (8, LANES))

    row_index = lax.broadcasted_iota(jnp.int32, (LANES, LANES), 0)
    col_index = lax.broadcasted_iota(jnp.int32, (LANES, LANES), 1)
    causal = row_index >= col_index
    lane_index = lax.broadcasted_iota(jnp.int32, (SPAN, LANES), 1)
    pair = LANES // head_size

    def inside(block):
        span = pl.ds(pl.multiple_of(block * SPAN, SPAN), SPAN)
        running = cum_buf[span, :]
        running_t = running.T
        steps_t = dt_ref[span, :].T
        scores = lax.dot_general(
            conv_bc[span, pl.ds(state, state)], conv_bc[span, pl.ds(0, state)],
            (((1,), (1,)), ((), ())), preferred_element_type=jnp.float32,
        )
        half = SPAN // 2
        for strip in range(width // LANES):
            lanes = pl.ds(strip * LANES, LANES)
            value = conv_x[span, lanes]
            upper, bottom, stacked_top, stacked = [], [], [], []
            for member in range(pair):
                head = strip * pair + member
                column = running[:, head : head + 1]
                line = running_t[head : head + 1, :]
                steps = steps_t[head : head + 1, :]

                def weights(r, c):
                    rs, cs = slice(r * half, (r + 1) * half), slice(c * half, (c + 1) * half)
                    gap = column[rs] - line[:, cs]
                    if r == c:
                        gap = jnp.where(causal, gap, -1e30)
                    return (scores[rs, cs] * jnp.exp(gap) * steps[:, cs]).astype(jnp.bfloat16)

                upper.append(weights(0, 0))
                bottom.extend([weights(1, 0), weights(1, 1)])
                own = jnp.where(lane_index // head_size == member, value, jnp.zeros_like(value))
                stacked_top.append(own[:half])
                stacked.append(own)
            top_out = jnp.dot(
                jnp.concatenate(upper, axis=1), jnp.concatenate(stacked_top, axis=0),
                preferred_element_type=jnp.float32,
            )
            bottom_out = jnp.dot(
                jnp.concatenate(bottom, axis=1), jnp.concatenate(stacked, axis=0),
                preferred_element_type=jnp.float32,
            )
            both = jnp.concatenate([top_out, bottom_out], axis=0)
            y_buf[span, lanes] = both + skip_ref[0:1, lanes] * value.astype(jnp.float32)

    sum_copies, rate_copies = [], []
    for o in range(1, devices):
        sum_copies.append(
            remote(
                sum_out.at[seq_peer[o]], sum_in.at[o], sum_send.at[o], sum_recv.at[o],
                "seq", seq_peer[o],
            )
        )
        rate_copies.append(
            remote(
                rate_out, rate_in.at[o], rate_send.at[o], rate_recv.at[o], "seq", seq_peer[o]
            )
        )
    for a, b in zip(sum_copies, rate_copies):
        b.start()
        a.start()

    early = max(blocks - 1, 1)

    def inside_step(block, carry):
        inside(block)
        return carry

    lax.fori_loop(0, early, inside_step, 0)

    for a, b in zip(sum_copies, rate_copies):
        b.wait()
        a.wait()
    sum_in[0] = sum_out[me]
    rate_in[0] = rate_out[...]

    running_state = jnp.zeros((share, width), jnp.float32)
    for i in range(devices):
        slot = lax.rem(me - i + devices, devices)
        carry_out[slot] = running_state.astype(jnp.bfloat16)
        decay = exact_dot(jnp.exp(rate_in[slot]), spread)[0:1]
        running_state = decay * running_state + sum_in[slot].astype(jnp.float32)

    carry_copies = []
    for o in range(1, devices):
        carry_copies.append(
            remote(
                carry_out.at[o], carry_in.at[o], carry_send.at[o], carry_recv.at[o],
                "seq", seq_back[o],
            )
        )
    for copy in carry_copies:
        copy.start()
    lax.fori_loop(early, blocks, inside_step, 0)
    for copy in carry_copies:
        copy.wait()
    carry_in[0] = carry_out[0]
    for j in range(devices):
        slot = lax.rem(j - me + devices, devices)
        carried[pl.ds(j * share, share), :] = carry_in[slot].astype(jnp.float32)

    squares = []
    for block in range(blocks):
        span = pl.ds(block * SPAN, SPAN)
        entry_decay = exact_dot(
            jnp.broadcast_to(jnp.exp(prefixes[block]), (8, LANES)), spread
        )[0:1]
        entering = (states[block] + entry_decay * carried[...]).astype(jnp.bfloat16)
        growth = jnp.exp(cum_buf[span, :])
        partial_sum = jnp.zeros((SPAN, LANES), jnp.float32)
        for strip in range(width // LANES):
            lanes = pl.ds(strip * LANES, LANES)
            column = slice(strip * LANES, (strip + 1) * LANES)
            cross = jnp.dot(
                conv_bc[span, pl.ds(state, state)], entering[:, column],
                preferred_element_type=jnp.float32,
            )
            scale = exact_dot(growth, spread[:, column])
            gated = (y_buf[span, lanes] + scale * cross) * silu(
                inner_ref[span, lanes].astype(jnp.float32)
            )
            y_buf[span, lanes] = gated
            partial_sum = partial_sum + gated * gated
        squares.append(jnp.sum(partial_sum.T, axis=0, keepdims=True))
    own_squares = jnp.concatenate(squares, axis=1)
    sq_out[...] = jnp.broadcast_to(own_squares, (8, rows))
    sq_copies = []
    for o in range(1, groups):
        sq_copies.append(
            remote(sq_out, sq_in.at[o], sq_send.at[o], sq_recv.at[o], "head", head_peer[o])
        )
    for copy in sq_copies:
        copy.start()
    for copy in sq_copies:
        copy.wait()
    total = own_squares
    for o in range(1, groups):
        total = total + sq_in[o, 0:1, :]
    inverse = lax.rsqrt(total / total_width + norm_floor)
    for block in range(blocks):
        part = jnp.broadcast_to(inverse[:, block * SPAN : (block + 1) * SPAN], (LANES, SPAN)).T
        span = pl.ds(block * SPAN, SPAN)
        for strip in range(width // LANES):
            lanes = pl.ds(strip * LANES, LANES)
            out_ref[span, lanes] = (y_buf[span, lanes] * part * gain_ref[0:1, lanes]).astype(
                jnp.bfloat16
            )


def scan_call(inner, bc, step_sizes, kernel_x, offset_x, kernel_bc, offset_bc, rate, skip, gain, head_size):
    devices, groups = lax.axis_size("seq"), lax.axis_size("head")
    rows, width = inner.shape[0], kernel_x.shape[1]
    state, taps = bc.shape[1] // 2, kernel_x.shape[0]
    blocks, share = rows // SPAN, state // devices
    sizes = (devices, groups, rows, width, state, taps, head_size)
    f32, bf16 = jnp.float32, jnp.bfloat16
    sem = pltpu.SemaphoreType.DMA
    return pl.pallas_call(
        functools.partial(scan_kernel, sizes),
        out_shape=jax.ShapeDtypeStruct((rows, width), bf16),
        in_specs=[pl.BlockSpec(memory_space=pltpu.VMEM)] * 10,
        out_specs=pl.BlockSpec(memory_space=pltpu.VMEM),
        scratch_shapes=[
            pltpu.VMEM((HALO, width), bf16),
            pltpu.VMEM((HALO, 2 * state), bf16),
            pltpu.VMEM((rows + 8, width), f32),
            pltpu.VMEM((rows + 8, 2 * state), f32),
            pltpu.VMEM((rows, width), bf16),
            pltpu.VMEM((rows, 2 * state), bf16),
            pltpu.VMEM((rows, width), f32),
            pltpu.VMEM((rows, LANES), f32),
            pltpu.VMEM((blocks + 1, state, width), f32),
            pltpu.VMEM((state, width), f32),
            pltpu.VMEM((devices, share, width), bf16),
            pltpu.VMEM((devices, share, width), bf16),
            pltpu.VMEM((8, LANES), f32),
            pltpu.VMEM((devices, 8, LANES), f32),
            pltpu.VMEM((devices, share, width), bf16),
            pltpu.VMEM((devices, share, width), bf16),
            pltpu.VMEM((8, rows), f32),
            pltpu.VMEM((groups, 8, rows), f32),
            sem((4,)),
            sem((devices,)),
            sem((devices,)),
            sem((devices,)),
            sem((devices,)),
            sem((devices,)),
            sem((devices,)),
            sem((groups,)),
            sem((groups,)),
        ],
        compiler_params=pltpu.CompilerParams(
            collective_id=0, has_side_effects=True, vmem_limit_bytes=60 * 1024 * 1024
        ),
    )(inner, bc, step_sizes, kernel_x, offset_x, kernel_bc, offset_bc, rate, skip, gain)


def on_device(
    tokens,
    pre_gain,
    inner_proj,
    outer_proj,
    kernel_x,
    kernel_bc,
    offset_x,
    offset_bc,
    dt_bias,
    a_log,
    skip_gain,
    norm_gain,
    out_proj,
):
    model_width = inner_proj.shape[0]
    local_width = inner_proj.shape[2]
    head_count = dt_bias.shape[0]
    head_size = local_width // head_count
    state_size = kernel_bc.shape[1] // 2
    joined_proj = inner_proj.reshape(model_width, 2 * local_width)
    normed = row_norm(lax.all_gather(tokens, "head", axis=0, tiled=True), pre_gain).astype(
        jnp.bfloat16
    )
    inner_part = jnp.dot(normed, joined_proj, preferred_element_type=jnp.float32).astype(
        jnp.bfloat16
    )
    outer_part = jnp.dot(normed, outer_proj, preferred_element_type=jnp.float32)
    head_index = lax.axis_index("head")
    dt_raw = lax.dynamic_slice_in_dim(
        outer_part, 2 * state_size + head_index * head_count, head_count, 1
    )
    lane_pad = LANES - head_count
    step_sizes = jnp.pad(jax.nn.softplus(dt_raw + dt_bias), ((0, 0), (0, lane_pad)))
    rate = jnp.pad(-jnp.exp(a_log), (0, lane_pad))[None]
    normed_out = scan_call(
        inner_part,
        outer_part[:, : 2 * state_size].astype(jnp.bfloat16),
        step_sizes,
        kernel_x,
        offset_x[None],
        kernel_bc,
        offset_bc[None],
        rate,
        jnp.repeat(skip_gain, head_size)[None],
        norm_gain[None],
        head_size,
    )
    return lax.psum_scatter(
        jnp.dot(normed_out, out_proj, preferred_element_type=jnp.float32).astype(jnp.bfloat16),
        "head",
        scatter_dimension=0,
        tiled=True,
    )


def solution(mesh):
    return jax.shard_map(
        on_device,
        mesh=mesh,
        in_specs=(
            P(("seq", "head"), None),
            P(),
            P(None, None, "head"),
            P(),
            P(None, "head"),
            P(),
            P("head"),
            P(),
            P("head"),
            P("head"),
            P("head"),
            P("head"),
            P("head", None),
        ),
        out_specs=P(("seq", "head"), None),
        check_vma=False,
    )
```
